32 devices in a mesh: row: 8 (over y, x, core), col: 4 (over z).
Axes of the slice: x: 2, y: 2, z: 4, core: 2. Of those that a mesh axis runs over, the one named last changes fastest.
Arguments:
- alignment_state: bfloat16 [128, 128, 256], P('col', 'row'), may hold values from -6 to 6
- layer_norm_gain: float32 [256], replicated, may hold values from 0.1 to 1.9
- left_weight_matrix: bfloat16 [256, 32], replicated, may hold values from -0.375 to 0.375
- right_weight_matrix: bfloat16 [256, 32], replicated, may hold values from -0.375 to 0.375
- output_weight_matrix: bfloat16 [1024, 128], replicated, may hold values from -0.1875 to 0.1875
- output_bias_vector: float32 [128], replicated, may hold values from -3 to 3
- pair_update_cotangent: bfloat16 [128, 128, 128], P('row', 'col'), may hold values from -40 to 40
Outputs:
- pair_update_output: bfloat16 [128, 128, 128], P('row', 'col')
- alignment_gradient: bfloat16 [128, 128, 256], P('col', 'row')
- left_weight_gradient: float32 [256, 32], replicated
- right_weight_gradient: float32 [256, 32], replicated
- out_w_grad: float32 [1024, 128], P(('row', 'col'))
- norm_gain_gradient: float32 [256], replicated
- output_bias_gradient: float32 [128], replicated
The draws below stay inside these ranges and needn't reach their ends.
All inputs are finite; a program needn't handle non-finite values.
Results may differ from the reference program's by a relative error of at most 0.024.
Values may be sent and summed in bfloat16 or wider, within the bound.
No kernel may reach another device: no remote copies, remote signals or barrier semaphores. Data moves between devices by JAX's collectives and lax.ppermute only.
A program may use at most 64 MiB of HBM per device.

```python
import jax
import jax.numpy as jnp
from jax import lax

ALIGNMENT_WIDTH = 256
PROJECTED_WIDTH = 32
PAIR_WIDTH = 128
ALIGNED_SEQUENCES = 128
CROP_RESIDUES = 128


def draw_pair_update_cotangent(key, part):
    first_key = jax.random.fold_in(jax.random.fold_in(key, 11), 0)
    ramp = 0.5 + jnp.arange(CROP_RESIDUES, dtype=jnp.float32) / CROP_RESIDUES
    profile = ramp[:, None, None] * ramp[None, :, None]
    base = jax.random.truncated_normal(first_key, -4.0, 4.0, (CROP_RESIDUES, CROP_RESIDUES, PAIR_WIDTH), jnp.float32)
    return (base * profile).astype(jnp.bfloat16)


def block_levels(stream_key, dims, pieces, smallest, top_value):
    gain = 1.0
    for axis_at, blocks in pieces:
        steps = jax.random.uniform(jax.random.fold_in(jax.random.fold_in(stream_key, 6), axis_at), (blocks,), jnp.float32, smallest / len(pieces), top_value / len(pieces))
        gain = gain * jnp.repeat(jnp.exp(steps), dims[axis_at] // blocks).reshape((-1,) + (1,) * (len(dims) - 1 - axis_at))
    return gain


def normal_values(rng, dims, scale, most, shards=(), kind=jnp.bfloat16):
    values = jax.random.normal(rng, dims, jnp.float32) * scale
    if len(shards) > 0:
        values = block_levels(rng, dims, shards, -0.22, 0.18) * values
    return jnp.clip(values, min=-most, max=most).astype(kind)


def setup_inputs(seed: int = 0) -> dict:
    key_list = jax.random.split(jax.random.key(seed), 8)
    return {
        "alignment_state": normal_values(key_list[0], (ALIGNED_SEQUENCES, CROP_RESIDUES, ALIGNMENT_WIDTH), 1.0, 6.0, ((0, 4), (1, 8))),
        "layer_norm_gain": jnp.clip(1.0 + 0.18 * jax.random.normal(key_list[1], (ALIGNMENT_WIDTH,), jnp.float32), 0.1, 1.9),
        "left_weight_matrix": normal_values(key_list[2], (ALIGNMENT_WIDTH, PROJECTED_WIDTH), ALIGNMENT_WIDTH ** -0.5, 0.375),
        "right_weight_matrix": normal_values(key_list[3], (ALIGNMENT_WIDTH, PROJECTED_WIDTH), ALIGNMENT_WIDTH ** -0.5, 0.375),
        "output_weight_matrix": normal_values(key_list[4], (PROJECTED_WIDTH * PROJECTED_WIDTH, PAIR_WIDTH), (PROJECTED_WIDTH * PROJECTED_WIDTH) ** -0.5, 0.1875),
        "output_bias_vector": normal_values(key_list[5], (PAIR_WIDTH,), 0.5, 3.0, (), jnp.float32),
        "pair_update_cotangent": draw_pair_update_cotangent(jax.random.fold_in(key_list[7], 71), 0),
    }


def apply_layer_norm(alignment_state):
    value_entries = alignment_state.astype(jnp.float32)
    center = value_entries - lax.optimization_barrier(jnp.mean(value_entries, axis=-1, keepdims=True))
    inverse_deviation = lax.rsqrt(lax.optimization_barrier(jnp.mean(center * center, axis=-1, keepdims=True)) + 1e-05)
    return (center * inverse_deviation, inverse_deviation)

def reference(alignment_state, layer_norm_gain, left_weight_matrix, right_weight_matrix, output_weight_matrix, output_bias_vector, pair_update_cotangent):
    normed_alignment, inverse_deviation = apply_layer_norm(alignment_state)
    layer_norm_output = (normed_alignment * layer_norm_gain).astype(jnp.bfloat16)
    normed_flat_rows = layer_norm_output.reshape(-1, ALIGNMENT_WIDTH)
    left_proj = jnp.dot(normed_flat_rows, left_weight_matrix, preferred_element_type=jnp.float32).astype(jnp.bfloat16).reshape(ALIGNED_SEQUENCES, CROP_RESIDUES, PROJECTED_WIDTH)
    right_proj = jnp.dot(normed_flat_rows, right_weight_matrix, preferred_element_type=jnp.float32).astype(jnp.bfloat16).reshape(ALIGNED_SEQUENCES, CROP_RESIDUES, PROJECTED_WIDTH)
    left_wide = left_proj.astype(jnp.float32)
    right_wide = right_proj.astype(jnp.float32)

    def visit(totals, row_start):
        right_acc, projection_running_sum = totals
        left_part = lax.dynamic_slice_in_dim(left_wide, row_start, 8, 1)
        cot_part = lax.dynamic_slice_in_dim(pair_update_cotangent, row_start, 8, 0)
        outer_prod = jnp.einsum('sic,sjd->ijcd', left_part, right_wide)
        outer_flat = (outer_prod / ALIGNED_SEQUENCES).astype(jnp.bfloat16).reshape(8 * CROP_RESIDUES, PROJECTED_WIDTH * PROJECTED_WIDTH)
        cot_flat = cot_part.reshape(8 * CROP_RESIDUES, PAIR_WIDTH)
        pair_part = (jnp.dot(outer_flat, output_weight_matrix, preferred_element_type=jnp.float32) + output_bias_vector).astype(jnp.bfloat16)
        projection_running_sum = projection_running_sum + jnp.dot(outer_flat.T, cot_flat, preferred_element_type=jnp.float32)
        outer_grad = jnp.dot(cot_flat, output_weight_matrix.T, preferred_element_type=jnp.float32).astype(jnp.bfloat16)
        outer_grad = outer_grad.astype(jnp.float32).reshape(8, CROP_RESIDUES, PROJECTED_WIDTH, PROJECTED_WIDTH)
        left_part_grad = jnp.einsum('ijcd,sjd->sic', outer_grad, right_wide) / ALIGNED_SEQUENCES
        right_acc = right_acc + jnp.einsum('ijcd,sic->sjd', outer_grad, left_part) / ALIGNED_SEQUENCES
        return ((right_acc, projection_running_sum), (pair_part.reshape(8, CROP_RESIDUES, PAIR_WIDTH), left_part_grad))
    starts = jnp.arange(CROP_RESIDUES // 8, dtype=jnp.int32) * 8
    initial = (jnp.zeros((ALIGNED_SEQUENCES, CROP_RESIDUES, PROJECTED_WIDTH), jnp.float32), jnp.zeros((PROJECTED_WIDTH * PROJECTED_WIDTH, PAIR_WIDTH), jnp.float32))
    (right_acc, projection_running_sum), (pair_parts, left_parts) = lax.scan(visit, initial, starts)
    pair_update_output = pair_parts.reshape(CROP_RESIDUES, CROP_RESIDUES, PAIR_WIDTH)
    left_d = jnp.transpose(left_parts, (1, 0, 2, 3)).reshape(ALIGNED_SEQUENCES, CROP_RESIDUES, PROJECTED_WIDTH).astype(jnp.bfloat16)
    right_d = right_acc.astype(jnp.bfloat16)
    left_flat = left_d.reshape(-1, PROJECTED_WIDTH)
    right_flat = right_d.reshape(-1, PROJECTED_WIDTH)
    normed_derivative = jnp.dot(left_flat, left_weight_matrix.T, preferred_element_type=jnp.float32) + jnp.dot(right_flat, right_weight_matrix.T, preferred_element_type=jnp.float32)
    normed_derivative = normed_derivative.reshape(ALIGNED_SEQUENCES, CROP_RESIDUES, ALIGNMENT_WIDTH)
    scaled_product = normed_derivative * layer_norm_gain
    alignment_gradient = ((scaled_product - lax.optimization_barrier(jnp.mean(scaled_product, axis=-1, keepdims=True)) - normed_alignment * lax.optimization_barrier(jnp.mean(scaled_product * normed_alignment, axis=-1, keepdims=True))) * inverse_deviation).astype(jnp.bfloat16)
    left_weight_gradient = jnp.dot(normed_flat_rows.T, left_flat, preferred_element_type=jnp.float32) / CROP_RESIDUES
    right_weight_gradient = jnp.dot(normed_flat_rows.T, right_flat, preferred_element_type=jnp.float32) / CROP_RESIDUES
    norm_gain_gradient = lax.optimization_barrier(jnp.sum(normed_derivative * normed_alignment, axis=(0, 1))) / CROP_RESIDUES
    output_bias_gradient = lax.optimization_barrier(jnp.sum(pair_update_cotangent.astype(jnp.float32), axis=(0, 1))) / CROP_RESIDUES
    return (pair_update_output, alignment_gradient, left_weight_gradient, right_weight_gradient, projection_running_sum / CROP_RESIDUES, norm_gain_gradient, output_bias_gradient)
```

```python
import functools

import jax
import jax.numpy as jnp
from jax import lax
from jax.experimental import pallas as pl
from jax.experimental.pallas import tpu as pltpu
from jax.sharding import PartitionSpec as P

F32, BF16 = jnp.float32, jnp.bfloat16
LANES = 128


def product(a, b, over=((1,), (0,))):
    return lax.dot_general(a, b, (over, ((), ())), preferred_element_type=F32)


def tree(terms):
    while len(terms) > 1:
        terms = [a + b for a, b in zip(terms[::2], terms[1::2])]
    return terms[0]


def wide(ref):
    return ref[...].astype(F32)


def call(name, body, args, outs, scratch=(), flops=1, limit=24):
    spec = pl.BlockSpec(memory_space=pltpu.VMEM)
    moved = sum(a.size * a.dtype.itemsize for a in args)
    return pl.pallas_call(
        body,
        out_shape=[jax.ShapeDtypeStruct(s, t) for s, t in outs],
        in_specs=[spec] * len(args),
        out_specs=[spec] * len(outs),
        scratch_shapes=list(scratch),
        name=name,
        cost_estimate=pl.CostEstimate(flops=flops, bytes_accessed=moved, transcendentals=0),
        compiler_params=pltpu.CompilerParams(vmem_limit_bytes=limit << 20),
    )(*args)


def normalize(rows):
    center = rows - jnp.mean(rows, axis=-1, keepdims=True)
    inverse = lax.rsqrt(jnp.mean(center * center, axis=-1, keepdims=True) + 1e-05)
    return center * inverse, inverse


def by_residue(x_ref, flat):
    seqs, residues, width = x_ref.shape
    values = wide(x_ref).reshape(seqs * residues, width)
    halves = range(width // LANES)
    for k in halves:
        flat[k] = values[:, k * LANES : (k + 1) * LANES]
    return [
        jnp.concatenate([flat[k, pl.ds(i, seqs, stride=residues), :] for k in halves], axis=1)
        for i in range(residues)
    ]


def channel_first(residues, chans):
    size = residues * chans
    source = lax.broadcasted_iota(jnp.int32, (size, size), 0)
    target = lax.broadcasted_iota(jnp.int32, (size, size), 1)
    place = (source % chans) * residues + source // chans
    return jnp.where(place == target, 1.0, 0.0).astype(BF16)


def project_kernel(chans, swap, x_ref, gain_ref, tiled_ref, out_ref, flat):
    seqs, residues, width = x_ref.shape
    rows = by_residue(x_ref, flat)
    normed, _ = normalize(jnp.concatenate(rows, axis=0))
    ln_out = (normed * gain_ref[...]).astype(F32)
    pack = LANES // chans
    lane = lax.broadcasted_iota(jnp.int32, (width, LANES), 1) // chans
    tiled = tiled_ref[...]
    weights = jnp.concatenate(
        [jnp.where(lane == k, tiled, jnp.zeros_like(tiled)) for k in range(pack)], axis=0
    )
    parts = []
    for g in range(residues // pack):
        piece = jnp.concatenate(
            [ln_out[(g * pack + k) * seqs : (g * pack + k + 1) * seqs] for k in range(pack)], axis=1
        )
        parts.append(product(piece.astype(BF16), weights))
    out = jnp.concatenate(parts, axis=1).astype(BF16)
    if swap:
        out = product(out, channel_first(residues, chans)).astype(BF16)
    out_ref[...] = out


def project(name, x, gain, tiled, chans, swap):
    seqs, residues, width = x.shape
    return call(
        name,
        functools.partial(project_kernel, chans, swap),
        (x, gain, tiled),
        [((seqs, residues * chans), BF16)],
        [pltpu.VMEM((width // LANES, seqs * residues, LANES), F32)],
        flops=40_000_000,
    )[0]


def spread_weight(w_ref, spread, chans):
    pack = LANES // chans
    pair_w = w_ref.shape[1]
    spread[...] = jnp.zeros_like(spread)
    for c in range(chans):
        block = w_ref[c * chans : (c + 1) * chans, :]
        for k in range(pack):
            row = c * LANES + k * chans
            spread[row : row + chans, k * pair_w : (k + 1) * pair_w] = block


def grad_kernel(chans, cot_ref, w_ref, og_ref, cotk_ref, bias_ref, flat, spread):
    residues, seconds, pair_w = cot_ref.shape
    pack = LANES // chans
    groups = seconds // pack
    cot = wide(cot_ref).reshape(residues * seconds, pair_w)
    flat[...] = cot
    bias_ref[...] = jnp.broadcast_to(jnp.sum(cot, axis=0, keepdims=True), bias_ref.shape)
    spread_weight(w_ref, spread, chans)
    for k in range(pack):
        rows = [flat[pl.ds(g * pack + k, residues, stride=seconds), :] for g in range(groups)]
        cotk_ref[k] = jnp.concatenate(rows, axis=0).astype(BF16)
    cot_wide = jnp.concatenate([cotk_ref[k] for k in range(pack)], axis=1)
    chunk = 8
    for first in range(0, chans, chunk):
        part = spread[first * LANES : (first + chunk) * LANES, :]
        out = product(cot_wide, part, ((1,), (1,))).astype(BF16)
        for c in range(chunk):
            for g in range(groups):
                row = (first + c) * residues
                og_ref[row : row + residues, g * LANES : (g + 1) * LANES] = out[
                    g * residues : (g + 1) * residues, c * LANES : (c + 1) * LANES
                ]


def places(ratio):
    row, col = lax.axis_index("row"), lax.axis_index("col")
    return row // ratio, row % ratio, col


def partial_kernel(cols, ratio, *refs):
    left_in, refs = refs[:cols], refs[cols:]
    right_in, refs = refs[: cols * ratio], refs[cols * ratio :]
    og_ref, refs = refs[0], refs[1:]
    left_out, refs = refs[:cols], refs[cols:]
    right_out, refs = refs[:ratio], refs[ratio:]
    left_all, right_all, left_sum, right_sum = refs
    seqs, width = left_in[0].shape
    total = seqs * cols
    q, h, z = places(ratio)
    for k in range(cols):
        left_all[pl.ds(pl.multiple_of((z ^ k) * seqs, seqs), seqs), :] = wide(left_in[k])
        for e in range(ratio):
            place = pl.ds(pl.multiple_of((q ^ k) * seqs, seqs), seqs)
            right_all[h ^ e, place, :] = wide(right_in[k * ratio + e])
    left = left_all[...].astype(BF16)
    sums = []
    for e in range(ratio):
        og = og_ref[:, e * width : (e + 1) * width]
        right_sum[e] = product(left, og) * (1.0 / total)
        sums.append(product(right_all[e].astype(BF16), og, ((1,), (1,))))
    left_sum[...] = sum(sums) * (1.0 / total)
    for k in range(cols):
        place = pl.ds(pl.multiple_of((z ^ k) * seqs, seqs), seqs)
        left_out[k][...] = left_sum[place, :].astype(BF16)
    for e in range(ratio):
        right_out[e][...] = right_sum[h ^ e].astype(BF16)


def forward_kernel(chans, ratio, *refs):
    left_ref, right_ref, cotk_ref, w_ref, bias_ref, pair_ref = refs[:6]
    proj_out, (flat, spread, facing, turned, proj) = refs[6 : 6 + ratio], refs[6 + ratio :]
    residues, seconds, pair_w = pair_ref.shape
    pack = LANES // chans
    groups = seconds // pack
    total = left_ref.shape[0]
    width = right_ref.shape[2]
    _, h, _ = places(ratio)
    spread_weight(w_ref, spread, chans)
    left = left_ref[...].astype(BF16)
    part = groups // ratio
    for e in range(ratio):
        outer = product(left, right_ref[e].astype(BF16), ((0,), (0,)))
        outer = (outer * (1.0 / total)).astype(BF16)
        for c in range(chans):
            for g in range(part):
                row = (e * part + g) * residues
                facing[row : row + residues, c * LANES : (c + 1) * LANES] = outer[
                    c * residues : (c + 1) * residues, g * LANES : (g + 1) * LANES
                ]
    pair = product(facing[...], spread[...])
    for g in range(groups):
        for k in range(pack):
            block = pair[g * residues : (g + 1) * residues, k * pair_w : (k + 1) * pair_w]
            flat[pl.ds(g * pack + k, residues, stride=seconds), :] = block + bias_ref[...]
    pair_ref[...] = flat[...].astype(BF16).reshape(residues, seconds, pair_w)
    size = groups * residues
    for c in range(chans):
        block = facing[:, c * LANES : (c + 1) * LANES].T
        for k in range(pack):
            turned[c * chans : (c + 1) * chans, k * size : (k + 1) * size] = block[
                k * chans : (k + 1) * chans
            ]
    cot = jnp.concatenate([cotk_ref[k] for k in range(pack)], axis=0)
    out = product(turned[...], cot)
    count, height = proj_out[0].shape[:2]
    proj[...] = out.reshape(count, ratio, height, pair_w)
    for e in range(ratio):
        for q in range(count):
            proj_out[e][q] = proj[q, h ^ e].astype(BF16)


def stacked(value, residues, chans):
    return jnp.concatenate(
        [value[:, i * chans : (i + 1) * chans] for i in range(residues)], axis=0
    )


def moment_kernel(cols, chans, *refs):
    left_in, right_in = refs[:cols], refs[cols : 2 * cols]
    x_ref, across_ref, bias_ref, left_ref, right_ref, stat_ref, flat = refs[2 * cols :]
    residues = x_ref.shape[1]
    width = x_ref.shape[2]
    left = tree([wide(r) for r in left_in]).astype(BF16)
    left = product(left, channel_first(residues, chans), ((1,), (1,)))
    right = tree([wide(r) for r in right_in])
    left_ref[...] = left.astype(BF16)
    right_ref[...] = right.astype(BF16)
    moments = []
    for value, rows_ref in ((left, x_ref), (right, across_ref)):
        normed, _ = normalize(jnp.concatenate(by_residue(rows_ref, flat), axis=0))
        value = stacked(value, residues, chans).astype(BF16)
        moments.append(product(value, normed.astype(BF16), ((0,), (0,))))
    moment = jnp.concatenate(moments, axis=0)
    halves = [moment[:, k * LANES : (k + 1) * LANES] for k in range(width // LANES)]
    bias = jnp.concatenate([bias_ref[...]] * 2, axis=0)
    stat_ref[...] = jnp.concatenate(halves + [bias], axis=0).astype(BF16)


def input_grad_kernel(chans, x_ref, gain_ref, lw_ref, rw_ref, left_ref, right_ref, out_ref, flat):
    seqs, residues, width = x_ref.shape
    normed, inverse = normalize(jnp.concatenate(by_residue(x_ref, flat), axis=0))
    left = stacked(wide(left_ref), residues, chans).astype(BF16)
    right = stacked(wide(right_ref), residues, chans).astype(BF16)
    ln_d = product(left, lw_ref[...], ((1,), (1,))) + product(right, rw_ref[...], ((1,), (1,)))
    scaled = ln_d * gain_ref[...]
    mean = jnp.mean(scaled, axis=-1, keepdims=True)
    tilt = jnp.mean(scaled * normed, axis=-1, keepdims=True)
    grad = (scaled - mean - normed * tilt) * inverse
    halves = range(width // LANES)
    for i in range(residues):
        for k in halves:
            piece = grad[i * seqs : (i + 1) * seqs, k * LANES : (k + 1) * LANES]
            flat[k, pl.ds(i, seqs, stride=residues), :] = piece
    values = jnp.concatenate([flat[k] for k in halves], axis=1)
    out_ref[...] = values.astype(BF16).reshape(seqs, residues, width)


def core_sum_kernel(ratio, *refs):
    right_in, refs = refs[:ratio], refs[ratio:]
    outs, flat = refs[:-1], refs[-1]
    seqs = outs[0].shape[0]
    q, _, _ = places(ratio)
    flat[...] = tree([wide(r) for r in right_in])
    for k, out in enumerate(outs):
        place = pl.ds(pl.multiple_of((q ^ k) * seqs, seqs), seqs)
        out[...] = flat[place, :].astype(BF16)


def first_stat_kernel(ratio, *refs):
    proj_in, stat_in = refs[:ratio], refs[ratio : 2 * ratio]
    outs, scratch = refs[2 * ratio : -1], refs[-1]
    height = scratch.shape[1]
    q, _, _ = places(ratio)
    scratch[...] = tree([wide(r) for r in proj_in])
    stat = tree([wide(r) for r in stat_in]).astype(BF16)
    for k, out in enumerate(outs):
        out[:height] = scratch[q ^ k].astype(BF16)
        out[height:] = stat


def second_stat_kernel(ratio, height, *refs):
    count = (len(refs) - 1) // 2
    ins, outs, scratch = refs[:count], refs[count : 2 * count], refs[-1]
    _, _, z = places(ratio)
    total = tree([wide(r) for r in ins])
    size = height * count
    scratch[...] = total[:size].reshape(scratch.shape)
    stat = total[size:].astype(BF16)
    for k, out in enumerate(outs):
        out[:height] = scratch[z ^ k].astype(BF16)
        out[height:] = stat


def last_stat_kernel(chans, height, scale, *refs):
    ins, (gain_ref, lw_ref, rw_ref) = refs[:-8], refs[-8:-5]
    left_ref, right_ref, proj_ref, norm_ref, bias_ref = refs[-5:]
    total = tree([wide(r) for r in ins]) * scale
    proj_ref[...] = total[:height]
    stat = total[height:]
    width = lw_ref.shape[0]
    size = 2 * chans
    halves = width // LANES
    moment = jnp.concatenate([stat[k * size : (k + 1) * size] for k in range(halves)], axis=1)
    moment = moment.T
    left, right = moment[:, :chans], moment[:, chans:]
    norm = left * wide(lw_ref) + right * wide(rw_ref)
    left_ref[...] = left * gain_ref[...]
    right_ref[...] = right * gain_ref[...]
    norm_ref[...] = jnp.sum(norm, axis=1, keepdims=True)
    bias_ref[...] = stat[halves * size : halves * size + 1]


def on_device(x, gain, left_w, right_w, out_w, bias, cot):
    seqs, residues, width = x.shape
    chans = left_w.shape[1]
    pair_w = out_w.shape[1]
    rows, cols = lax.axis_size("row"), lax.axis_size("col")
    ratio = rows // cols
    seconds = residues * ratio
    total_seqs, total_res = seqs * cols, residues * rows
    wide_proj, wide_pair = residues * chans, seconds * chans
    pack = LANES // chans
    groups = seconds // pack
    gain_row = gain.reshape(1, width)

    def col_swap(value, k):
        return lax.ppermute(value, "col", [(i, i ^ k) for i in range(cols)])

    def chip_swap(value, k):
        return lax.ppermute(value, "row", [(i, i ^ (k * ratio)) for i in range(rows)])

    def core_swap(value, e):
        return lax.ppermute(value, "row", [(i, i ^ e) for i in range(rows)])

    def across(value):
        pairs = [
            ((q * ratio + h) * cols + z, (z * ratio + h) * cols + q)
            for q in range(cols)
            for h in range(ratio)
            for z in range(cols)
        ]
        return lax.ppermute(value, ("row", "col"), pairs)

    x_across = across(x)
    left_own = project("left", x, gain_row, jnp.tile(left_w, (1, pack)), chans, True)
    left_in = [left_own] + [col_swap(left_own, k) for k in range(1, cols)]
    og, cotk, bias_part = call(
        "outer_grad",
        functools.partial(grad_kernel, chans),
        (cot, out_w),
        [
            ((chans * residues, wide_pair), BF16),
            ((pack, groups * residues, pair_w), BF16),
            ((8, pair_w), F32),
        ],
        [
            pltpu.VMEM((residues * seconds, pair_w), F32),
            pltpu.VMEM((chans * LANES, pack * pair_w), BF16),
        ],
        flops=540_000_000,
    )
    right_own = project("right", x_across, gain_row, jnp.tile(right_w, (1, pack)), chans, False)
    right_in = []
    for k in range(cols):
        chip = right_own if k == 0 else chip_swap(right_own, k)
        right_in += [chip] + [core_swap(chip, e) for e in range(1, ratio)]

    outs = call(
        "partials",
        functools.partial(partial_kernel, cols, ratio),
        (*left_in, *right_in, og),
        [((seqs, wide_proj), BF16)] * cols
        + [((total_seqs, wide_proj), BF16)] * ratio
        + [((total_seqs, wide_proj), F32), ((ratio, total_seqs, wide_proj), F32)],
        [
            pltpu.VMEM((total_seqs, wide_proj), F32),
            pltpu.VMEM((ratio, total_seqs, wide_proj), F32),
        ],
        flops=270_000_000,
    )
    left_parts, right_parts = outs[:cols], outs[cols : cols + ratio]
    left_all, right_all = outs[cols + ratio :]

    right_core = [right_parts[0]] + [core_swap(right_parts[e], e) for e in range(1, ratio)]
    left_parts = [left_parts[0]] + [col_swap(left_parts[k], k) for k in range(1, cols)]
    right_parts = call(
        "core_sum",
        functools.partial(core_sum_kernel, ratio),
        right_core,
        [((seqs, wide_proj), BF16)] * cols,
        [pltpu.VMEM((total_seqs, wide_proj), F32)],
    )
    right_parts = [right_parts[0]] + [chip_swap(right_parts[k], k) for k in range(1, cols)]

    block = chans * chans // rows
    outs = call(
        "forward",
        functools.partial(forward_kernel, chans, ratio),
        (left_all, right_all, cotk, out_w, bias.reshape(1, pair_w)),
        [((residues, seconds, pair_w), BF16)] + [((cols, block, pair_w), BF16)] * ratio,
        [
            pltpu.VMEM((residues * seconds, pair_w), F32),
            pltpu.VMEM((chans * LANES, pack * pair_w), BF16),
            pltpu.VMEM((groups * residues, chans * LANES), BF16),
            pltpu.VMEM((chans * chans, pack * groups * residues), BF16),
            pltpu.VMEM((cols, ratio, block, pair_w), F32),
        ],
        flops=800_000_000,
        limit=32,
    )
    pair_update, proj_parts = outs[0], outs[1:]
    proj_core = [proj_parts[0]] + [core_swap(proj_parts[e], e) for e in range(1, ratio)]

    stat_rows = 2 * chans * (width // LANES) + 16
    left_d, right_d, stat = call(
        "moments",
        functools.partial(moment_kernel, cols, chans),
        (*left_parts, *right_parts, x, x_across, bias_part),
        [((seqs, wide_proj), BF16), ((seqs, wide_proj), BF16), ((stat_rows, LANES), BF16)],
        [pltpu.VMEM((width // LANES, seqs * residues, LANES), F32)],
    )
    stat_core = [stat] + [core_swap(stat, e) for e in range(1, ratio)]
    right_home = across(right_d)
    firsts = call(
        "first_stat",
        functools.partial(first_stat_kernel, ratio),
        (*proj_core, *stat_core),
        [((block + stat_rows, pair_w), BF16)] * cols,
        [pltpu.VMEM((cols, block, pair_w), F32)],
    )
    firsts = [firsts[0]] + [chip_swap(firsts[k], k) for k in range(1, cols)]
    height = block // cols
    seconds_out = call(
        "second_stat",
        functools.partial(second_stat_kernel, ratio, height),
        firsts,
        [((height + stat_rows, pair_w), BF16)] * cols,
        [pltpu.VMEM((cols, height, pair_w), F32)],
    )
    seconds_out = [seconds_out[0]] + [col_swap(seconds_out[k], k) for k in range(1, cols)]
    grad = call(
        "input_grad",
        functools.partial(input_grad_kernel, chans),
        (x, gain_row, left_w, right_w, left_d, right_home),
        [((seqs, residues, width), BF16)],
        [pltpu.VMEM((width // LANES, seqs * residues, LANES), F32)],
    )[0]
    left_g, right_g, proj_g, norm_g, bias_g = call(
        "last_stat",
        functools.partial(last_stat_kernel, chans, height, 1.0 / total_res),
        (*seconds_out, gain.reshape(width, 1), left_w, right_w),
        [
            ((width, chans), F32),
            ((width, chans), F32),
            ((height, pair_w), F32),
            ((width, 1), F32),
            ((1, pair_w), F32),
        ],
    )
    return (
        pair_update,
        grad,
        left_g,
        right_g,
        proj_g,
        norm_g.reshape(width),
        bias_g.reshape(pair_w),
    )


def solution(mesh):
    return jax.shard_map(
        on_device,
        mesh=mesh,
        in_specs=(P("col", "row", None), P(), P(), P(), P(), P(), P("row", "col", None)),
        out_specs=(
            P("row", "col", None),
            P("col", "row", None),
            P(),
            P(),
            P(("row", "col"), None),
            P(),
            P(),
        ),
        check_vma=False,
    )
```

```python
import functools

import jax
import jax.numpy as jnp
from jax import lax
from jax.experimental import pallas as pl
from jax.experimental.pallas import tpu as pltpu
from jax.sharding import PartitionSpec as P


F32, BF16 = jnp.float32, jnp.bfloat16
LANES = 128


def product(a, b, over=((1,), (0,))):
    return lax.dot_general(a, b, (over, ((), ())), preferred_element_type=F32)


def tree(terms):
    while len(terms) > 1:
        terms = [a + b for a, b in zip(terms[::2], terms[1::2])]
    return terms[0]


def wide(ref):
    return ref[...].astype(F32)


def call(body, args, outs, scratch=(), flops=1, limit=24, far=0):
    spec = pl.BlockSpec(memory_space=pltpu.VMEM)
    args = [
        pltpu.with_memory_space_constraint(a, pltpu.HBM) if n < far else a
        for n, a in enumerate(args)
    ]
    moved = sum(a.size * a.dtype.itemsize for a in args)
    return pl.pallas_call(
        body,
        out_shape=[jax.ShapeDtypeStruct(d, t) for d, t in outs],
        in_specs=[pl.BlockSpec(memory_space=pltpu.HBM)] * far + [spec] * (len(args) - far),
        out_specs=[spec] * len(outs),
        scratch_shapes=list(scratch),
        cost_estimate=pl.CostEstimate(flops=flops, bytes_accessed=moved, transcendentals=0),
        compiler_params=pltpu.CompilerParams(vmem_limit_bytes=limit << 20),
    )(*args)


def normalize(rows):
    center = rows - jnp.mean(rows, axis=-1, keepdims=True)
    inverse = lax.rsqrt(jnp.mean(center * center, axis=-1, keepdims=True) + 1e-05)
    return center * inverse, inverse


def by_residue(x_ref, flat):
    seqs, residues, width = x_ref.shape
    values = wide(x_ref).reshape(seqs * residues, width)
    halves = range(width // LANES)
    for k in halves:
        flat[k] = values[:, k * LANES : (k + 1) * LANES]
    return [
        jnp.concatenate([flat[k, pl.ds(i, seqs, stride=residues), :] for k in halves], axis=1)
        for i in range(residues)
    ]


def channel_first(residues, chans):
    size = residues * chans
    source = lax.broadcasted_iota(jnp.int32, (size, size), 0)
    target = lax.broadcasted_iota(jnp.int32, (size, size), 1)
    place = (source % chans) * residues + source // chans
    return jnp.where(place == target, 1.0, 0.0).astype(BF16)


def fetch(pairs, sems):
    copies = [
        pltpu.make_async_copy(source, target, sems.at[n])
        for n, (source, target) in enumerate(pairs)
    ]
    for copy in copies:
        copy.start()
    return copies


def project_kernel(chans, *refs):
    count = (len(refs) - 4) // 2
    sources, targets = refs[:count], refs[count : 2 * count]
    left_ref, right_ref, flat, sems = refs[2 * count :]
    copies = fetch(zip(sources, targets), sems)
    for copy in copies[:4]:
        copy.wait()
    x_in, gain_in = targets[:2]
    seqs, residues, _ = x_in.shape
    normed, _ = normalize(jnp.concatenate(by_residue(x_in, flat), axis=0))
    ln_out = normed * gain_in[...]
    pack = LANES // chans
    places = []
    for weight_in in targets[2:4]:
        weight = weight_in[...]
        zero = jnp.zeros_like(weight)
        places += [
            jnp.concatenate([weight if k == m else zero for m in range(pack)], axis=1)
            for k in range(pack)
        ]
    weights = jnp.concatenate(places, axis=0)
    left, right = [], []
    for g in range(residues // pack):
        piece = jnp.concatenate(
            [ln_out[(g * pack + k) * seqs : (g * pack + k + 1) * seqs] for k in range(pack)], axis=1
        )
        both = product(piece.astype(BF16), weights, ((1,), (1,)))
        left.append(both[:, :LANES])
        right.append(both[:, LANES:])
    right_ref[...] = jnp.concatenate(right, axis=1).astype(BF16)
    left = jnp.concatenate(left, axis=1).astype(BF16)
    left_ref[...] = product(left, channel_first(residues, chans)).astype(BF16)
    for copy in copies[4:]:
        copy.wait()


def spread_weight(w_ref, spread, chans):
    pack = LANES // chans
    pair_w = w_ref.shape[1]
    spread[...] = jnp.zeros_like(spread)
    for c in range(chans):
        block = w_ref[c * chans : (c + 1) * chans, :]
        for k in range(pack):
            row = c * LANES + k * chans
            spread[row : row + chans, k * pair_w : (k + 1) * pair_w] = block


def grad_kernel(chans, cot_ref, w_ref, og_ref, cotk_ref, bias_ref, flat, spread):
    residues, seconds, pair_w = cot_ref.shape
    pack = LANES // chans
    groups = seconds // pack
    cot = wide(cot_ref).reshape(residues * seconds, pair_w)
    flat[...] = cot
    bias_ref[...] = jnp.broadcast_to(jnp.sum(cot, axis=0, keepdims=True), bias_ref.shape)
    spread_weight(w_ref, spread, chans)
    for k in range(pack):
        rows = [flat[pl.ds(g * pack + k, residues, stride=seconds), :] for g in range(groups)]
        cotk_ref[k] = jnp.concatenate(rows, axis=0).astype(BF16)
    cot_wide = jnp.concatenate([cotk_ref[k] for k in range(pack)], axis=1)
    chunk = 8
    for first in range(0, chans, chunk):
        part = spread[first * LANES : (first + chunk) * LANES, :]
        out = product(cot_wide, part, ((1,), (1,))).astype(BF16)
        for c in range(chunk):
            for g in range(groups):
                row = (first + c) * residues
                og_ref[row : row + residues, g * LANES : (g + 1) * LANES] = out[
                    g * residues : (g + 1) * residues, c * LANES : (c + 1) * LANES
                ]


def places(ratio):
    row, col = lax.axis_index("row"), lax.axis_index("col")
    return row // ratio, row % ratio, col


def right_grad_kernel(cols, ratio, *refs):
    left_in, og_ref = refs[:cols], refs[cols]
    outs, (all_ref, gathered, sums) = refs[cols + 1 : cols + 1 + ratio], refs[cols + 1 + ratio :]
    seqs, width = left_in[0].shape
    _, h, z = places(ratio)
    for k in range(cols):
        gathered[pl.ds(pl.multiple_of((z ^ k) * seqs, seqs), seqs), :] = wide(left_in[k])
    left = gathered[...].astype(BF16)
    all_ref[...] = left
    for e in range(ratio):
        sums[e] = product(left, og_ref[:, e * width : (e + 1) * width]) * (1.0 / (seqs * cols))
    for e in range(ratio):
        outs[e][...] = sums[h ^ e].astype(BF16)


def left_grad_kernel(cols, ratio, *refs):
    right_in, og_ref = refs[: cols * ratio], refs[cols * ratio]
    outs, (all_ref, gathered, sums) = refs[cols * ratio + 1 : -3], refs[-3:]
    seqs, width = right_in[0].shape
    q, h, z = places(ratio)
    for k in range(cols):
        place = pl.ds(pl.multiple_of((q ^ k ^ (cols - 1)) * seqs, seqs), seqs)
        for e in range(ratio):
            gathered[h ^ e, place, :] = wide(right_in[k * ratio + e])
    parts = []
    for e in range(ratio):
        right = gathered[e].astype(BF16)
        all_ref[e] = right
        parts.append(product(right, og_ref[:, e * width : (e + 1) * width], ((1,), (1,))))
    sums[...] = sum(parts) * (1.0 / (seqs * cols))
    for k in range(cols):
        place = pl.ds(pl.multiple_of((z ^ k) * seqs, seqs), seqs)
        outs[k][...] = sums[place, :].astype(BF16)


def forward_kernel(chans, ratio, *refs):
    left_ref, right_ref, cotk_ref, w_ref, bias_ref, pair_ref = refs[:6]
    proj_out, (flat, spread, facing, turned, proj) = refs[6 : 6 + ratio], refs[6 + ratio :]
    residues, seconds, pair_w = pair_ref.shape
    pack = LANES // chans
    groups = seconds // pack
    total = left_ref.shape[0]
    _, h, _ = places(ratio)
    spread_weight(w_ref, spread, chans)
    left = left_ref[...]
    part = groups // ratio
    for e in range(ratio):
        outer = product(left, right_ref[e], ((0,), (0,)))
        outer = (outer * (1.0 / total)).astype(BF16)
        for c in range(chans):
            for g in range(part):
                row = (e * part + g) * residues
                facing[row : row + residues, c * LANES : (c + 1) * LANES] = outer[
                    c * residues : (c + 1) * residues, g * LANES : (g + 1) * LANES
                ]
    pair = product(facing[...], spread[...])
    for g in range(groups):
        for k in range(pack):
            block = pair[g * residues : (g + 1) * residues, k * pair_w : (k + 1) * pair_w]
            flat[pl.ds(g * pack + k, residues, stride=seconds), :] = block + bias_ref[...]
    pair_ref[...] = flat[...].astype(BF16).reshape(residues, seconds, pair_w)
    size = groups * residues
    for c in range(chans):
        block = facing[:, c * LANES : (c + 1) * LANES].T
        for k in range(pack):
            turned[c * chans : (c + 1) * chans, k * size : (k + 1) * size] = block[
                k * chans : (k + 1) * chans
            ]
    cot = jnp.concatenate([cotk_ref[k] for k in range(pack)], axis=0)
    out = product(turned[...], cot)
    count, height = proj_out[0].shape[:2]
    proj[...] = out.reshape(count, ratio, height, pair_w)
    for e in range(ratio):
        for q in range(count):
            proj_out[e][q] = proj[q, h ^ e].astype(BF16)


def stacked(value, residues, chans):
    return jnp.concatenate(
        [value[:, i * chans : (i + 1) * chans] for i in range(residues)], axis=0
    )


def moment_kernel(cols, chans, *refs):
    left_in, (right_ref, x_ref, bias_ref, left_ref, stat_ref, flat) = refs[:cols], refs[cols:]
    residues, width = x_ref.shape[1:]
    normed, _ = normalize(jnp.concatenate(by_residue(x_ref, flat), axis=0))
    left = tree([wide(r) for r in left_in]).astype(BF16)
    left = product(left, channel_first(residues, chans), ((1,), (1,)))
    left_ref[...] = left.astype(BF16)
    both = [stacked(value, residues, chans) for value in (left, wide(right_ref))]
    both = jnp.concatenate(both, axis=1).astype(BF16)
    moment = product(both, normed.astype(BF16), ((0,), (0,)))
    halves = [moment[:, k * LANES : (k + 1) * LANES] for k in range(width // LANES)]
    bias = jnp.concatenate([bias_ref[...]] * 2, axis=0)
    stat_ref[...] = jnp.concatenate(halves + [bias], axis=0).astype(BF16)


def sum_kernel(*refs):
    refs[-1][...] = tree([wide(r) for r in refs[:-1]]).astype(BF16)


def input_grad_kernel(chans, x_ref, gain_ref, lw_ref, rw_ref, left_ref, right_ref, out_ref, flat):
    seqs, residues, width = x_ref.shape
    normed, inverse = normalize(jnp.concatenate(by_residue(x_ref, flat), axis=0))
    left = stacked(wide(left_ref), residues, chans).astype(BF16)
    right = stacked(wide(right_ref), residues, chans).astype(BF16)
    ln_d = product(left, lw_ref[...]) + product(right, rw_ref[...])
    scaled = ln_d * gain_ref[...]
    mean = jnp.mean(scaled, axis=-1, keepdims=True)
    tilt = jnp.mean(scaled * normed, axis=-1, keepdims=True)
    grad = (scaled - mean - normed * tilt) * inverse
    halves = range(width // LANES)
    for i in range(residues):
        for k in halves:
            piece = grad[i * seqs : (i + 1) * seqs, k * LANES : (k + 1) * LANES]
            flat[k, pl.ds(i, seqs, stride=residues), :] = piece
    values = jnp.concatenate([flat[k] for k in halves], axis=1)
    out_ref[...] = values.astype(BF16).reshape(seqs, residues, width)


def core_sum_kernel(ratio, *refs):
    right_in, refs = refs[:ratio], refs[ratio:]
    outs, flat = refs[:-1], refs[-1]
    seqs = outs[0].shape[0]
    q, _, _ = places(ratio)
    flat[...] = tree([wide(r) for r in right_in])
    for k, out in enumerate(outs):
        place = pl.ds(pl.multiple_of((q ^ k ^ (len(outs) - 1)) * seqs, seqs), seqs)
        out[...] = flat[place, :].astype(BF16)


def first_stat_kernel(ratio, *refs):
    proj_in, stat_in = refs[:ratio], refs[ratio : 2 * ratio]
    outs, scratch = refs[2 * ratio : -1], refs[-1]
    height = scratch.shape[1]
    q, _, _ = places(ratio)
    scratch[...] = tree([wide(r) for r in proj_in])
    stat = tree([wide(r) for r in stat_in]).astype(BF16)
    for k, out in enumerate(outs):
        out[:height] = scratch[q ^ k].astype(BF16)
        out[height:] = stat


def second_stat_kernel(ratio, height, *refs):
    count = (len(refs) - 1) // 2
    ins, outs, scratch = refs[:count], refs[count : 2 * count], refs[-1]
    _, _, z = places(ratio)
    total = tree([wide(r) for r in ins])
    size = height * count
    scratch[...] = total[:size].reshape(scratch.shape)
    stat = total[size:].astype(BF16)
    for k, out in enumerate(outs):
        out[:height] = scratch[z ^ k].astype(BF16)
        out[height:] = stat


def last_stat_kernel(chans, height, scale, *refs):
    ins, (gain_ref, lw_ref, rw_ref) = refs[:-8], refs[-8:-5]
    left_ref, right_ref, proj_ref, norm_ref, bias_ref = refs[-5:]
    total = tree([wide(r) for r in ins]) * scale
    proj_ref[...] = total[:height]
    stat = total[height:]
    width = lw_ref.shape[1]
    size = 2 * chans
    halves = width // LANES
    moment = jnp.concatenate([stat[k * size : (k + 1) * size] for k in range(halves)], axis=1)
    left, right = moment[:chans], moment[chans:]
    norm_ref[...] = jnp.sum(left * wide(lw_ref) + right * wide(rw_ref), axis=0, keepdims=True)
    left_ref[...] = left * gain_ref[...]
    right_ref[...] = right * gain_ref[...]
    bias_ref[...] = stat[halves * size : halves * size + 1]


def whole_step(x, gain, left_w, right_w, out_w, bias, cot):
    seqs, residues, width = x.shape
    chans = left_w.shape[1]
    pair_w = out_w.shape[1]
    rows, cols = lax.axis_size("row"), lax.axis_size("col")
    ratio = rows // cols
    seconds = residues * ratio
    total_seqs, total_res = seqs * cols, residues * rows
    wide_proj, wide_pair = residues * chans, seconds * chans
    pack = LANES // chans
    groups = seconds // pack
    gain_row = gain.reshape(1, width)
    left_t, right_t = left_w.T, right_w.T

    def cols_of(parts):
        pairs = [[(i, i ^ k) for i in range(cols)] for k in range(cols)]
        return [parts[0]] + [lax.ppermute(parts[k], "col", pairs[k]) for k in range(1, cols)]

    def chips_of(parts):
        pairs = [[(i, i ^ (k * ratio)) for i in range(rows)] for k in range(cols)]
        return [parts[0]] + [lax.ppermute(parts[k], "row", pairs[k]) for k in range(1, cols)]

    def cores_of(parts):
        pairs = [[(i, i ^ e) for i in range(rows)] for e in range(ratio)]
        return [parts[0]] + [lax.ppermute(parts[e], "row", pairs[e]) for e in range(1, ratio)]

    pairs = [
        ((q * ratio + h) * cols + z, ((z ^ (cols - 1)) * ratio + h) * cols + q)
        for q in range(cols)
        for h in range(ratio)
        for z in range(cols)
    ]

    sources = (x, gain_row, left_t, right_t, cot, out_w, bias.reshape(1, pair_w))
    outs = call(
        functools.partial(project_kernel, chans),
        sources,
        [(a.shape, a.dtype) for a in sources] + [((seqs, wide_proj), BF16)] * 2,
        [
            pltpu.VMEM((width // LANES, seqs * residues, LANES), F32),
            pltpu.SemaphoreType.DMA((len(sources),)),
        ],
        flops=40_000_000,
        far=len(sources),
    )
    x, gain_row, left_t, right_t, cot, out_w, bias_row = outs[:-2]
    left_own, right_own = outs[-2:]
    right_own = lax.ppermute(right_own, ("row", "col"), pairs)
    left_in = cols_of([left_own] * cols)
    og, cotk, bias_part = call(
        functools.partial(grad_kernel, chans),
        (cot, out_w),
        [
            ((chans * residues, wide_pair), BF16),
            ((pack, groups * residues, pair_w), BF16),
            ((8, pair_w), F32),
        ],
        [
            pltpu.VMEM((residues * seconds, pair_w), F32),
            pltpu.VMEM((chans * LANES, pack * pair_w), BF16),
        ],
        flops=540_000_000,
    )
    right_in = []
    for chip in chips_of([right_own] * cols):
        right_in += cores_of([chip] * ratio)

    outs = call(
        functools.partial(right_grad_kernel, cols, ratio),
        (*left_in, og),
        [((total_seqs, wide_proj), BF16)] * (ratio + 1),
        [
            pltpu.VMEM((total_seqs, wide_proj), F32),
            pltpu.VMEM((ratio, total_seqs, wide_proj), F32),
        ],
        flops=134_000_000,
    )
    right_parts, left_all = outs[:ratio], outs[ratio]
    right_parts = call(
        functools.partial(core_sum_kernel, ratio),
        cores_of(right_parts),
        [((seqs, wide_proj), BF16)] * cols,
        [pltpu.VMEM((total_seqs, wide_proj), F32)],
    )
    right_parts = chips_of(right_parts)
    right_sent = call(sum_kernel, right_parts, [((seqs, wide_proj), BF16)])[0]
    right_d = lax.ppermute(right_sent, ("row", "col"), [(b, a) for a, b in pairs])

    outs = call(
        functools.partial(left_grad_kernel, cols, ratio),
        (*right_in, og),
        [((seqs, wide_proj), BF16)] * cols + [((ratio, total_seqs, wide_proj), BF16)],
        [
            pltpu.VMEM((ratio, total_seqs, wide_proj), F32),
            pltpu.VMEM((total_seqs, wide_proj), F32),
        ],
        flops=134_000_000,
    )
    left_parts, right_all = outs[:cols], outs[cols]
    left_parts = cols_of(left_parts)

    block = chans * chans // rows
    outs = call(
        functools.partial(forward_kernel, chans, ratio),
        (left_all, right_all, cotk, out_w, bias_row),
        [((residues, seconds, pair_w), BF16)] + [((cols, block, pair_w), BF16)] * ratio,
        [
            pltpu.VMEM((residues * seconds, pair_w), F32),
            pltpu.VMEM((chans * LANES, pack * pair_w), BF16),
            pltpu.VMEM((groups * residues, chans * LANES), BF16),
            pltpu.VMEM((chans * chans, pack * groups * residues), BF16),
            pltpu.VMEM((cols, ratio, block, pair_w), F32),
        ],
        flops=800_000_000,
        limit=32,
    )
    pair_update, proj_parts = outs[0], outs[1:]
    proj_core = cores_of(proj_parts)

    stat_rows = 2 * chans * (width // LANES) + 16
    left_d, stat = call(
        functools.partial(moment_kernel, cols, chans),
        (*left_parts, right_d, x, bias_part),
        [((seqs, wide_proj), BF16), ((stat_rows, LANES), BF16)],
        [pltpu.VMEM((width // LANES, seqs * residues, LANES), F32)],
    )
    stat_core = cores_of([stat] * ratio)
    firsts = call(
        functools.partial(first_stat_kernel, ratio),
        (*proj_core, *stat_core),
        [((block + stat_rows, pair_w), BF16)] * cols,
        [pltpu.VMEM((cols, block, pair_w), F32)],
    )
    firsts = chips_of(firsts)
    height = block // cols
    seconds_out = call(
        functools.partial(second_stat_kernel, ratio, height),
        firsts,
        [((height + stat_rows, pair_w), BF16)] * cols,
        [pltpu.VMEM((cols, height, pair_w), F32)],
    )
    seconds_out = cols_of(seconds_out)
    grad = call(
        functools.partial(input_grad_kernel, chans),
        (x, gain_row, left_t, right_t, left_d, right_d),
        [((seqs, residues, width), BF16)],
        [pltpu.VMEM((width // LANES, seqs * residues, LANES), F32)],
    )[0]
    left_g, right_g, proj_g, norm_g, bias_g = call(
        functools.partial(last_stat_kernel, chans, height, 1.0 / total_res),
        (*seconds_out, gain_row, left_t, right_t),
        [
            ((chans, width), F32),
            ((chans, width), F32),
            ((height, pair_w), F32),
            ((1, width), F32),
            ((1, pair_w), F32),
        ],
    )
    return (
        pair_update,
        grad,
        left_g.T,
        right_g.T,
        proj_g,
        norm_g.reshape(width),
        bias_g.reshape(pair_w),
    )


def solution(mesh):
    return jax.shard_map(
        whole_step,
        mesh=mesh,
        in_specs=(P("col", "row", None), P(), P(), P(), P(), P(), P("row", "col", None)),
        out_specs=(
            P("row", "col", None),
            P("col", "row", None),
            P(),
            P(),
            P(("row", "col"), None),
            P(),
            P(),
        ),
        check_vma=False,
    )
```

```python
import functools

import jax
import jax.numpy as jnp
from jax import lax
from jax.experimental import pallas as pl
from jax.experimental.pallas import tpu as pltpu
from jax.sharding import PartitionSpec as P


F32, BF16 = jnp.float32, jnp.bfloat16
LANES = 128


def product(a, b, over=((1,), (0,))):
    return lax.dot_general(a, b, (over, ((), ())), preferred_element_type=F32)


def tree(terms):
    while len(terms) > 1:
        terms = [a + b for a, b in zip(terms[::2], terms[1::2])]
    return terms[0]


def wide(ref):
    return ref[...].astype(F32)


def call(body, args, outs, scratch=(), flops=1, limit=24, far=0):
    spec = pl.BlockSpec(memory_space=pltpu.VMEM)
    args = [
        pltpu.with_memory_space_constraint(a, pltpu.HBM) if n < far else a
        for n, a in enumerate(args)
    ]
    moved = sum(a.size * a.dtype.itemsize for a in args)
    return pl.pallas_call(
        body,
        out_shape=[jax.ShapeDtypeStruct(d, t) for d, t in outs],
        in_specs=[pl.BlockSpec(memory_space=pltpu.HBM)] * far + [spec] * (len(args) - far),
        out_specs=[spec] * len(outs),
        scratch_shapes=list(scratch),
        cost_estimate=pl.CostEstimate(flops=flops, bytes_accessed=moved, transcendentals=0),
        compiler_params=pltpu.CompilerParams(vmem_limit_bytes=limit << 20),
    )(*args)


def normalize(rows):
    center = rows - jnp.mean(rows, axis=-1, keepdims=True)
    inverse = lax.rsqrt(jnp.mean(center * center, axis=-1, keepdims=True) + 1e-05)
    return center * inverse, inverse


def by_residue(x_ref, flat):
    seqs, residues, width = x_ref.shape
    values = wide(x_ref).reshape(seqs * residues, width)
    halves = range(width // LANES)
    for k in halves:
        flat[k] = values[:, k * LANES : (k + 1) * LANES]
    return [
        jnp.concatenate([flat[k, pl.ds(i, seqs, stride=residues), :] for k in halves], axis=1)
        for i in range(residues)
    ]


def channel_first(residues, chans):
    size = residues * chans
    source = lax.broadcasted_iota(jnp.int32, (size, size), 0)
    target = lax.broadcasted_iota(jnp.int32, (size, size), 1)
    place = (source & (chans - 1)) * residues + (source >> (chans.bit_length() - 1))
    return jnp.where(place == target, 1.0, 0.0).astype(BF16)


def fetch(pairs, sems):
    copies = [
        pltpu.make_async_copy(source, target, sems.at[n])
        for n, (source, target) in enumerate(pairs)
    ]
    for copy in copies:
        copy.start()
    return copies


def stacked(value, residues, chans):
    return jnp.concatenate(
        [value[:, i * chans : (i + 1) * chans] for i in range(residues)], axis=0
    )


def unstacked(value, residues, seqs):
    return jnp.concatenate(
        [value[i * seqs : (i + 1) * seqs] for i in range(residues)], axis=1
    )


def project_kernel(chans, *refs):
    count = (len(refs) - 6) // 2
    sources, targets = refs[:count], refs[count : 2 * count]
    left_ref, right_ref, normed_ref, order_ref, flat, sems = refs[2 * count :]
    copies = fetch(zip(sources, targets), sems)
    order_ref[...] = channel_first(sources[0].shape[1], chans)
    for copy in copies[:4]:
        copy.wait()
    x_in, gain_in = targets[:2]
    seqs, residues, _ = x_in.shape
    normed, _ = normalize(jnp.concatenate(by_residue(x_in, flat), axis=0))
    ln_out = normed * gain_in[...]
    normed_ref[...] = normed.astype(BF16)
    weights = jnp.concatenate([weight[...] for weight in targets[2:4]], axis=0)
    both = product(ln_out.astype(BF16), weights, ((1,), (1,)))
    right_ref[...] = unstacked(both[:, chans:], residues, seqs).astype(BF16)
    left = unstacked(both[:, :chans], residues, seqs).astype(BF16)
    left_ref[...] = product(left, order_ref[...]).astype(BF16)
    for copy in copies[4:]:
        copy.wait()


def pieces(block, chans):
    return [block[:, k * chans : (k + 1) * chans] for k in range(block.shape[1] // chans)]


def grad_kernel(chans, cot_ref, w_ref, og_ref, cotk_ref, bias_ref, flat):
    residues, seconds, pair_w = cot_ref.shape
    pack = LANES // chans
    groups = seconds // pack
    size = groups * residues
    cot = wide(cot_ref).reshape(residues * seconds, pair_w)
    flat[...] = cot
    bias_ref[...] = jnp.broadcast_to(jnp.sum(cot, axis=0, keepdims=True), bias_ref.shape)
    for k in range(pack):
        rows = [flat[pl.ds(g * pack + k, residues, stride=seconds), :] for g in range(groups)]
        cotk_ref[k * size : (k + 1) * size] = jnp.concatenate(rows, axis=0).astype(BF16)
    out = product(cotk_ref[...], w_ref[...], ((1,), (1,))).astype(BF16)
    parts = [pieces(out[k * size : (k + 1) * size], chans) for k in range(pack)]
    for c in range(chans):
        block = jnp.concatenate([parts[k][c] for k in range(pack)], axis=1)
        for g in range(groups):
            og_ref[c * residues : (c + 1) * residues, g * LANES : (g + 1) * LANES] = block[
                g * residues : (g + 1) * residues
            ]


def places(ratio):
    row, col = lax.axis_index("row"), lax.axis_index("col")
    return row // ratio, row % ratio, col


def right_grad_kernel(cols, ratio, *refs):
    left_in, og_ref = refs[:cols], refs[cols]
    outs, (all_ref, gathered, sums) = refs[cols + 1 : cols + 1 + ratio], refs[cols + 1 + ratio :]
    seqs, width = left_in[0].shape
    _, h, z = places(ratio)
    for k in range(cols):
        gathered[pl.ds(pl.multiple_of((z ^ k) * seqs, seqs), seqs), :] = wide(left_in[k])
    left = gathered[...].astype(BF16)
    all_ref[...] = left
    for e in range(ratio):
        sums[e] = product(left, og_ref[:, e * width : (e + 1) * width]) * (1.0 / (seqs * cols))
    for e in range(ratio):
        outs[e][...] = sums[h ^ e].astype(BF16)


def left_grad_kernel(cols, ratio, *refs):
    right_in, og_ref = refs[: cols * ratio], refs[cols * ratio]
    outs, (all_ref, gathered, sums) = refs[cols * ratio + 1 : -3], refs[-3:]
    seqs, width = right_in[0].shape
    q, h, z = places(ratio)
    for k in range(cols):
        place = pl.ds(pl.multiple_of((q ^ k ^ (cols - 1)) * seqs, seqs), seqs)
        for e in range(ratio):
            gathered[h ^ e, place, :] = wide(right_in[k * ratio + e])
    parts = []
    for e in range(ratio):
        right = gathered[e].astype(BF16)
        all_ref[e] = right
        parts.append(product(right, og_ref[:, e * width : (e + 1) * width], ((1,), (1,))))
    sums[...] = sum(parts) * (1.0 / (seqs * cols))
    for k in range(cols):
        place = pl.ds(pl.multiple_of((z ^ k) * seqs, seqs), seqs)
        outs[k][...] = sums[place, :].astype(BF16)


def spread_weight(w_ref, spread, chans):
    pack = LANES // chans
    pair_w = w_ref.shape[1]
    spread[...] = jnp.zeros_like(spread)
    for c in range(chans):
        block = w_ref[c * chans : (c + 1) * chans, :]
        for k in range(pack):
            row = c * LANES + k * chans
            spread[row : row + chans, k * pair_w : (k + 1) * pair_w] = block


def forward_kernel(chans, ratio, *refs):
    left_ref, right_ref, cotk_ref, w_ref, bias_ref, pair_ref = refs[:6]
    proj_out, (flat, spread, facing, turned, proj) = refs[6 : 6 + ratio], refs[6 + ratio :]
    residues, seconds, pair_w = pair_ref.shape
    pack = LANES // chans
    groups = seconds // pack
    total = left_ref.shape[0]
    _, h, _ = places(ratio)
    spread_weight(w_ref, spread, chans)
    left = left_ref[...]
    part = groups // ratio
    for e in range(ratio):
        outer = product(left, right_ref[e], ((0,), (0,)))
        outer = (outer * (1.0 / total)).astype(BF16)
        for c in range(chans):
            for g in range(part):
                row = (e * part + g) * residues
                facing[row : row + residues, c * LANES : (c + 1) * LANES] = outer[
                    c * residues : (c + 1) * residues, g * LANES : (g + 1) * LANES
                ]
    pair = product(facing[...], spread[...])
    for g in range(groups):
        for k in range(pack):
            block = pair[g * residues : (g + 1) * residues, k * pair_w : (k + 1) * pair_w]
            flat[pl.ds(g * pack + k, residues, stride=seconds), :] = block + bias_ref[...]
    pair_ref[...] = flat[...].astype(BF16).reshape(residues, seconds, pair_w)
    size = groups * residues
    for c in range(chans):
        block = facing[:, c * LANES : (c + 1) * LANES].T
        for k in range(pack):
            turned[c * chans : (c + 1) * chans, k * size : (k + 1) * size] = block[
                k * chans : (k + 1) * chans
            ]
    out = product(turned[...], cotk_ref[...])
    count, height = proj_out[0].shape[:2]
    proj[...] = out.reshape(count, ratio, height, pair_w)
    for e in range(ratio):
        for q in range(count):
            proj_out[e][q] = proj[q, h ^ e].astype(BF16)


def moment_kernel(cols, chans, *refs):
    left_in, (right_ref, normed_ref, order_ref, bias_ref, left_ref, stat_ref) = (
        refs[:cols],
        refs[cols:],
    )
    residues, width = right_ref.shape[1] // chans, normed_ref.shape[1]
    left = tree([wide(r) for r in left_in]).astype(BF16)
    left = product(left, order_ref[...], ((1,), (1,)))
    left_ref[...] = left.astype(BF16)
    both = [stacked(value, residues, chans) for value in (left, wide(right_ref))]
    both = jnp.concatenate(both, axis=1).astype(BF16)
    moment = product(both, normed_ref[...], ((0,), (0,)))
    halves = [moment[:, k * LANES : (k + 1) * LANES] for k in range(width // LANES)]
    stat_ref[...] = jnp.concatenate(halves + [bias_ref[...]], axis=0).astype(BF16)


def sum_kernel(*refs):
    refs[-1][...] = tree([wide(r) for r in refs[:-1]]).astype(BF16)


def input_grad_kernel(chans, x_ref, gain_ref, lw_ref, rw_ref, left_ref, right_ref, out_ref, flat):
    seqs, residues, width = x_ref.shape
    normed, inverse = normalize(jnp.concatenate(by_residue(x_ref, flat), axis=0))
    left = stacked(wide(left_ref), residues, chans).astype(BF16)
    right = stacked(wide(right_ref), residues, chans).astype(BF16)
    ln_d = product(left, lw_ref[...]) + product(right, rw_ref[...])
    scaled = ln_d * gain_ref[...]
    mean = jnp.mean(scaled, axis=-1, keepdims=True)
    tilt = jnp.mean(scaled * normed, axis=-1, keepdims=True)
    grad = (scaled - mean - normed * tilt) * inverse
    halves = range(width // LANES)
    for i in range(residues):
        for k in halves:
            piece = grad[i * seqs : (i + 1) * seqs, k * LANES : (k + 1) * LANES]
            flat[k, pl.ds(i, seqs, stride=residues), :] = piece
    values = jnp.concatenate([flat[k] for k in halves], axis=1)
    out_ref[...] = values.astype(BF16).reshape(seqs, residues, width)


def core_sum_kernel(ratio, *refs):
    right_in, refs = refs[:ratio], refs[ratio:]
    outs, flat = refs[:-1], refs[-1]
    seqs = outs[0].shape[0]
    q, _, _ = places(ratio)
    flat[...] = tree([wide(r) for r in right_in])
    for k, out in enumerate(outs):
        place = pl.ds(pl.multiple_of((q ^ k ^ (len(outs) - 1)) * seqs, seqs), seqs)
        out[...] = flat[place, :].astype(BF16)


def first_stat_kernel(ratio, *refs):
    proj_in, stat_in = refs[:ratio], refs[ratio : 2 * ratio]
    outs, scratch = refs[2 * ratio : -1], refs[-1]
    height = scratch.shape[1]
    q, _, _ = places(ratio)
    scratch[...] = tree([wide(r) for r in proj_in])
    stat = tree([wide(r) for r in stat_in]).astype(BF16)
    for k, out in enumerate(outs):
        out[:height] = scratch[q ^ k].astype(BF16)
        out[height:] = stat


def second_stat_kernel(ratio, height, *refs):
    count = (len(refs) - 1) // 2
    ins, outs, scratch = refs[:count], refs[count : 2 * count], refs[-1]
    _, _, z = places(ratio)
    total = tree([wide(r) for r in ins])
    size = height * count
    scratch[...] = total[:size].reshape(scratch.shape)
    stat = total[size:].astype(BF16)
    for k, out in enumerate(outs):
        out[:height] = scratch[z ^ k].astype(BF16)
        out[height:] = stat


def last_stat_kernel(chans, height, scale, *refs):
    ins, (gain_ref, lw_ref, rw_ref) = refs[:-8], refs[-8:-5]
    left_ref, right_ref, proj_ref, norm_ref, bias_ref = refs[-5:]
    total = tree([wide(r) for r in ins]) * scale
    proj_ref[...] = total[:height]
    stat = total[height:]
    width = lw_ref.shape[1]
    size = 2 * chans
    halves = width // LANES
    moment = jnp.concatenate([stat[k * size : (k + 1) * size] for k in range(halves)], axis=1)
    left, right = moment[:chans], moment[chans:]
    norm_ref[...] = jnp.sum(left * wide(lw_ref) + right * wide(rw_ref), axis=0, keepdims=True)
    left_ref[...] = left * gain_ref[...]
    right_ref[...] = right * gain_ref[...]
    bias_ref[...] = stat[halves * size : halves * size + 1]


def whole_step(x, gain, left_w, right_w, out_w, bias, cot):
    seqs, residues, width = x.shape
    chans = left_w.shape[1]
    pair_w = out_w.shape[1]
    rows, cols = lax.axis_size("row"), lax.axis_size("col")
    ratio = rows // cols
    seconds = residues * ratio
    total_seqs, total_res = seqs * cols, residues * rows
    wide_proj, wide_pair = residues * chans, seconds * chans
    pack = LANES // chans
    groups = seconds // pack
    gain_row = gain.reshape(1, width)
    left_t, right_t = left_w.T, right_w.T

    def cols_of(parts):
        pairs = [[(i, i ^ k) for i in range(cols)] for k in range(cols)]
        return [parts[0]] + [lax.ppermute(parts[k], "col", pairs[k]) for k in range(1, cols)]

    def chips_of(parts):
        pairs = [[(i, i ^ (k * ratio)) for i in range(rows)] for k in range(cols)]
        return [parts[0]] + [lax.ppermute(parts[k], "row", pairs[k]) for k in range(1, cols)]

    def cores_of(parts):
        pairs = [[(i, i ^ e) for i in range(rows)] for e in range(ratio)]
        return [parts[0]] + [lax.ppermute(parts[e], "row", pairs[e]) for e in range(1, ratio)]

    pairs = [
        ((q * ratio + h) * cols + z, ((z ^ (cols - 1)) * ratio + h) * cols + q)
        for q in range(cols)
        for h in range(ratio)
        for z in range(cols)
    ]

    sources = (x, gain_row, left_t, right_t, cot, out_w, bias.reshape(1, pair_w))
    outs = call(
        functools.partial(project_kernel, chans),
        sources,
        [(a.shape, a.dtype) for a in sources]
        + [((seqs, wide_proj), BF16)] * 2
        + [((residues * seqs, width), BF16), ((wide_proj, wide_proj), BF16)],
        [
            pltpu.VMEM((width // LANES, seqs * residues, LANES), F32),
            pltpu.SemaphoreType.DMA((len(sources),)),
        ],
        flops=40_000_000,
        far=len(sources),
    )
    x, gain_row, left_t, right_t, cot, out_w, bias_row = outs[: len(sources)]
    left_own, right_own, normed, order = outs[len(sources) :]
    right_own = lax.ppermute(right_own, ("row", "col"), pairs)
    left_in = cols_of([left_own] * cols)
    og, cotk, bias_part = call(
        functools.partial(grad_kernel, chans),
        (cot, out_w),
        [
            ((chans * residues, wide_pair), BF16),
            ((pack * groups * residues, pair_w), BF16),
            ((8, pair_w), F32),
        ],
        [pltpu.VMEM((residues * seconds, pair_w), F32)],
        flops=540_000_000,
    )
    right_in = []
    for chip in chips_of([right_own] * cols):
        right_in += cores_of([chip] * ratio)

    outs = call(
        functools.partial(right_grad_kernel, cols, ratio),
        (*left_in, og),
        [((total_seqs, wide_proj), BF16)] * (ratio + 1),
        [
            pltpu.VMEM((total_seqs, wide_proj), F32),
            pltpu.VMEM((ratio, total_seqs, wide_proj), F32),
        ],
        flops=134_000_000,
    )
    right_parts, left_all = outs[:ratio], outs[ratio]
    right_parts = call(
        functools.partial(core_sum_kernel, ratio),
        cores_of(right_parts),
        [((seqs, wide_proj), BF16)] * cols,
        [pltpu.VMEM((total_seqs, wide_proj), F32)],
    )
    right_parts = chips_of(right_parts)
    right_sent = call(sum_kernel, right_parts, [((seqs, wide_proj), BF16)])[0]
    right_d = lax.ppermute(right_sent, ("row", "col"), [(b, a) for a, b in pairs])

    outs = call(
        functools.partial(left_grad_kernel, cols, ratio),
        (*right_in, og),
        [((seqs, wide_proj), BF16)] * cols + [((ratio, total_seqs, wide_proj), BF16)],
        [
            pltpu.VMEM((ratio, total_seqs, wide_proj), F32),
            pltpu.VMEM((total_seqs, wide_proj), F32),
        ],
        flops=134_000_000,
    )
    left_parts, right_all = outs[:cols], outs[cols]
    left_parts = cols_of(left_parts)

    block = chans * chans // rows
    outs = call(
        functools.partial(forward_kernel, chans, ratio),
        (left_all, right_all, cotk, out_w, bias_row),
        [((residues, seconds, pair_w), BF16)] + [((cols, block, pair_w), BF16)] * ratio,
        [
            pltpu.VMEM((residues * seconds, pair_w), F32),
            pltpu.VMEM((chans * LANES, pack * pair_w), BF16),
            pltpu.VMEM((groups * residues, chans * LANES), BF16),
            pltpu.VMEM((chans * chans, pack * groups * residues), BF16),
            pltpu.VMEM((cols, ratio, block, pair_w), F32),
        ],
        flops=800_000_000,
        limit=32,
    )
    pair_update, proj_parts = outs[0], outs[1:]
    proj_core = cores_of(proj_parts)

    stat_rows = 2 * chans * (width // LANES) + 8
    left_d, stat = call(
        functools.partial(moment_kernel, cols, chans),
        (*left_parts, right_d, normed, order, bias_part),
        [((seqs, wide_proj), BF16), ((stat_rows, LANES), BF16)],
    )
    stat_core = cores_of([stat] * ratio)
    firsts = call(
        functools.partial(first_stat_kernel, ratio),
        (*proj_core, *stat_core),
        [((block + stat_rows, pair_w), BF16)] * cols,
        [pltpu.VMEM((cols, block, pair_w), F32)],
    )
    firsts = chips_of(firsts)
    height = block // cols
    seconds_out = call(
        functools.partial(second_stat_kernel, ratio, height),
        firsts,
        [((height + stat_rows, pair_w), BF16)] * cols,
        [pltpu.VMEM((cols, height, pair_w), F32)],
    )
    seconds_out = cols_of(seconds_out)
    grad = call(
        functools.partial(input_grad_kernel, chans),
        (x, gain_row, left_t, right_t, left_d, right_d),
        [((seqs, residues, width), BF16)],
        [pltpu.VMEM((width // LANES, seqs * residues, LANES), F32)],
    )[0]
    left_g, right_g, proj_g, norm_g, bias_g = call(
        functools.partial(last_stat_kernel, chans, height, 1.0 / total_res),
        (*seconds_out, gain_row, left_t, right_t),
        [
            ((chans, width), F32),
            ((chans, width), F32),
            ((height, pair_w), F32),
            ((1, width), F32),
            ((1, pair_w), F32),
        ],
    )
    return (
        pair_update,
        grad,
        left_g.T,
        right_g.T,
        proj_g,
        norm_g.reshape(width),
        bias_g.reshape(pair_w),
    )


def solution(mesh):
    return jax.shard_map(
        whole_step,
        mesh=mesh,
        in_specs=(P("col", "row", None), P(), P(), P(), P(), P(), P("row", "col", None)),
        out_specs=(
            P("row", "col", None),
            P("col", "row", None),
            P(),
            P(),
            P(("row", "col"), None),
            P(),
            P(),
        ),
        check_vma=False,
    )
```

```python
import functools

import jax
import jax.numpy as jnp
from jax import lax
from jax.experimental import pallas as pl
from jax.experimental.pallas import tpu as pltpu
from jax.sharding import PartitionSpec as P


F32, BF16 = jnp.float32, jnp.bfloat16
LANES = 128


def product(a, b, over=((1,), (0,))):
    return lax.dot_general(a, b, (over, ((), ())), preferred_element_type=F32)


def tree(terms):
    while len(terms) > 1:
        terms = [a + b for a, b in zip(terms[::2], terms[1::2])]
    return terms[0]


def wide(ref):
    return ref[...].astype(F32)


def call(body, args, outs, scratch=(), flops=1, limit=24, far=0):
    spec = pl.BlockSpec(memory_space=pltpu.VMEM)
    args = [
        pltpu.with_memory_space_constraint(a, pltpu.HBM) if n < far else a
        for n, a in enumerate(args)
    ]
    moved = sum(a.size * a.dtype.itemsize for a in args)
    return pl.pallas_call(
        body,
        out_shape=[jax.ShapeDtypeStruct(d, t) for d, t in outs],
        in_specs=[pl.BlockSpec(memory_space=pltpu.HBM)] * far + [spec] * (len(args) - far),
        out_specs=[spec] * len(outs),
        scratch_shapes=list(scratch),
        cost_estimate=pl.CostEstimate(flops=flops, bytes_accessed=moved, transcendentals=0),
        compiler_params=pltpu.CompilerParams(vmem_limit_bytes=limit << 20),
    )(*args)


def normalize(rows):
    center = rows - jnp.mean(rows, axis=-1, keepdims=True)
    inverse = lax.rsqrt(jnp.mean(center * center, axis=-1, keepdims=True) + 1e-05)
    return center * inverse, inverse


def by_residue(x_ref, flat):
    seqs, residues, width = x_ref.shape
    values = wide(x_ref).reshape(seqs * residues, width)
    halves = range(width // LANES)
    for k in halves:
        flat[k] = values[:, k * LANES : (k + 1) * LANES]
    return [
        jnp.concatenate([flat[k, pl.ds(i, seqs, stride=residues), :] for k in halves], axis=1)
        for i in range(residues)
    ]


def channel_first(residues, chans):
    size = residues * chans
    source = lax.broadcasted_iota(jnp.int32, (size, size), 0)
    target = lax.broadcasted_iota(jnp.int32, (size, size), 1)
    place = (source & (chans - 1)) * residues + (source >> (chans.bit_length() - 1))
    return jnp.where(place == target, 1.0, 0.0).astype(BF16)


def fetch(pairs, sems):
    copies = [
        pltpu.make_async_copy(source, target, sems.at[n])
        for n, (source, target) in enumerate(pairs)
    ]
    for copy in copies:
        copy.start()
    return copies


def stacked(value, residues, chans):
    return jnp.concatenate(
        [value[:, i * chans : (i + 1) * chans] for i in range(residues)], axis=0
    )


def unstacked(value, residues, seqs):
    return jnp.concatenate(
        [value[i * seqs : (i + 1) * seqs] for i in range(residues)], axis=1
    )


def project_kernel(chans, *refs):
    count = (len(refs) - 6) // 2
    sources, targets = refs[:count], refs[count : 2 * count]
    left_ref, right_ref, normed_ref, order_ref, flat, sems = refs[2 * count :]
    copies = fetch(zip(sources, targets), sems)
    order_ref[...] = channel_first(sources[0].shape[1], chans)
    for copy in copies[:4]:
        copy.wait()
    x_in, gain_in = targets[:2]
    seqs, residues, _ = x_in.shape
    normed, _ = normalize(jnp.concatenate(by_residue(x_in, flat), axis=0))
    ln_out = normed * gain_in[...]
    normed_ref[...] = normed.astype(BF16)
    weights = jnp.concatenate([weight[...] for weight in targets[2:4]], axis=0)
    both = product(ln_out.astype(BF16), weights, ((1,), (1,)))
    right_ref[...] = unstacked(both[:, chans:], residues, seqs).astype(BF16)
    left = unstacked(both[:, :chans], residues, seqs).astype(BF16)
    left_ref[...] = product(left, order_ref[...]).astype(BF16)
    for copy in copies[4:]:
        copy.wait()


def pieces(block, chans):
    return [block[:, k * chans : (k + 1) * chans] for k in range(block.shape[1] // chans)]


def grad_kernel(chans, cot_ref, w_ref, og_ref, cotk_ref, bias_ref, flat):
    residues, seconds, pair_w = cot_ref.shape
    pack = LANES // chans
    groups = seconds // pack
    size = groups * residues
    cot = wide(cot_ref).reshape(residues * seconds, pair_w)
    flat[...] = cot
    bias_ref[...] = jnp.broadcast_to(jnp.sum(cot, axis=0, keepdims=True), bias_ref.shape)
    for k in range(pack):
        rows = [flat[pl.ds(g * pack + k, residues, stride=seconds), :] for g in range(groups)]
        cotk_ref[k * size : (k + 1) * size] = jnp.concatenate(rows, axis=0).astype(BF16)
    out = product(cotk_ref[...], w_ref[...], ((1,), (1,))).astype(BF16)
    parts = [pieces(out[k * size : (k + 1) * size], chans) for k in range(pack)]
    for c in range(chans):
        block = jnp.concatenate([parts[k][c] for k in range(pack)], axis=1)
        for g in range(groups):
            og_ref[c * residues : (c + 1) * residues, g * LANES : (g + 1) * LANES] = block[
                g * residues : (g + 1) * residues
            ]


def places(ratio):
    row, col = lax.axis_index("row"), lax.axis_index("col")
    return row // ratio, row % ratio, col


def order_of(bits):
    order = [0]
    for bit in bits:
        order = order + [k ^ bit for k in order]
    return order


def right_grad_kernel(cols, ratio, *refs):
    left_in, og_ref = refs[:cols], refs[cols]
    outs, (all_ref, gathered, sums) = refs[cols + 1 : cols + 1 + ratio], refs[cols + 1 + ratio :]
    seqs, width = left_in[0].shape
    _, h, z = places(ratio)
    for k in range(cols):
        gathered[pl.ds(pl.multiple_of((z ^ k) * seqs, seqs), seqs), :] = wide(left_in[k])
    left = gathered[...].astype(BF16)
    all_ref[...] = left
    for e in range(ratio):
        sums[e] = product(left, og_ref[:, e * width : (e + 1) * width]) * (1.0 / (seqs * cols))
    for e in range(ratio):
        outs[e][...] = sums[h ^ e].astype(BF16)


def left_grad_kernel(cols, ratio, *refs):
    right_in, og_ref = refs[: cols * ratio], refs[cols * ratio]
    outs, (all_ref, gathered, sums) = refs[cols * ratio + 1 : -3], refs[-3:]
    seqs, width = right_in[0].shape
    q, h, z = places(ratio)
    for k in range(cols):
        place = pl.ds(pl.multiple_of((q ^ k ^ (cols - 1)) * seqs, seqs), seqs)
        for e in range(ratio):
            gathered[h ^ e, place, :] = wide(right_in[k * ratio + e])
    parts = []
    for e in range(ratio):
        right = gathered[e].astype(BF16)
        all_ref[e] = right
        parts.append(product(right, og_ref[:, e * width : (e + 1) * width], ((1,), (1,))))
    sums[...] = sum(parts) * (1.0 / (seqs * cols))
    for k in range(cols):
        place = pl.ds(pl.multiple_of((z ^ k) * seqs, seqs), seqs)
        outs[k][...] = sums[place, :].astype(BF16)


def spread_weight(w_ref, spread, chans):
    pack = LANES // chans
    pair_w = w_ref.shape[1]
    spread[...] = jnp.zeros_like(spread)
    for c in range(chans):
        block = w_ref[c * chans : (c + 1) * chans, :]
        for k in range(pack):
            row = c * LANES + k * chans
            spread[row : row + chans, k * pair_w : (k + 1) * pair_w] = block


def forward_kernel(chans, ratio, *refs):
    left_ref, right_ref, cotk_ref, w_ref, bias_ref, pair_ref = refs[:6]
    proj_out, (flat, spread, facing, turned, proj) = refs[6 : 6 + ratio], refs[6 + ratio :]
    residues, seconds, pair_w = pair_ref.shape
    pack = LANES // chans
    groups = seconds // pack
    total = left_ref.shape[0]
    _, h, _ = places(ratio)
    spread_weight(w_ref, spread, chans)
    left = left_ref[...]
    part = groups // ratio
    for e in range(ratio):
        outer = product(left, right_ref[e], ((0,), (0,)))
        outer = (outer * (1.0 / total)).astype(BF16)
        for c in range(chans):
            for g in range(part):
                row = (e * part + g) * residues
                facing[row : row + residues, c * LANES : (c + 1) * LANES] = outer[
                    c * residues : (c + 1) * residues, g * LANES : (g + 1) * LANES
                ]
    pair = product(facing[...], spread[...])
    for g in range(groups):
        for k in range(pack):
            block = pair[g * residues : (g + 1) * residues, k * pair_w : (k + 1) * pair_w]
            flat[pl.ds(g * pack + k, residues, stride=seconds), :] = block + bias_ref[...]
    pair_ref[...] = flat[...].astype(BF16).reshape(residues, seconds, pair_w)
    size = groups * residues
    for c in range(chans):
        block = facing[:, c * LANES : (c + 1) * LANES].T
        for k in range(pack):
            turned[c * chans : (c + 1) * chans, k * size : (k + 1) * size] = block[
                k * chans : (k + 1) * chans
            ]
    out = product(turned[...], cotk_ref[...])
    count, height = proj_out[0].shape[:2]
    proj[...] = out.reshape(count, ratio, height, pair_w)
    for e in range(ratio):
        for q in range(count):
            proj_out[e][q] = proj[q, h ^ e].astype(BF16)


def moment_kernel(cols, chans, *refs):
    left_in, (right_ref, normed_ref, order_ref, bias_ref, left_ref, stat_ref) = (
        refs[:cols],
        refs[cols:],
    )
    residues, width = right_ref.shape[1] // chans, normed_ref.shape[1]
    left = tree([wide(r) for r in left_in]).astype(BF16)
    left = product(left, order_ref[...], ((1,), (1,)))
    left_ref[...] = left.astype(BF16)
    both = [stacked(value, residues, chans) for value in (left, wide(right_ref))]
    both = jnp.concatenate(both, axis=1).astype(BF16)
    moment = product(both, normed_ref[...], ((0,), (0,)))
    halves = [moment[:, k * LANES : (k + 1) * LANES] for k in range(width // LANES)]
    stat_ref[...] = jnp.concatenate(halves + [bias_ref[...]], axis=0).astype(BF16)


def split_kernel(*refs):
    total = tree([wide(r) for r in refs[:2]])
    outs = refs[2:]
    size = outs[0].shape[0]
    for n, out in enumerate(outs):
        out[...] = total[n * size : (n + 1) * size].astype(BF16)


def input_grad_kernel(chans, x_ref, gain_ref, lw_ref, rw_ref, left_ref, right_ref, out_ref, flat):
    seqs, residues, width = x_ref.shape
    normed, inverse = normalize(jnp.concatenate(by_residue(x_ref, flat), axis=0))
    left = stacked(wide(left_ref), residues, chans).astype(BF16)
    right = stacked(wide(right_ref), residues, chans).astype(BF16)
    ln_d = product(left, lw_ref[...]) + product(right, rw_ref[...])
    scaled = ln_d * gain_ref[...]
    mean = jnp.mean(scaled, axis=-1, keepdims=True)
    tilt = jnp.mean(scaled * normed, axis=-1, keepdims=True)
    grad = (scaled - mean - normed * tilt) * inverse
    halves = range(width // LANES)
    for i in range(residues):
        for k in halves:
            piece = grad[i * seqs : (i + 1) * seqs, k * LANES : (k + 1) * LANES]
            flat[k, pl.ds(i, seqs, stride=residues), :] = piece
    values = jnp.concatenate([flat[k] for k in halves], axis=1)
    out_ref[...] = values.astype(BF16).reshape(seqs, residues, width)


def core_sum_kernel(order, ratio, *refs):
    right_in, outs, flat = refs[:ratio], refs[ratio:-1], refs[-1]
    cols = len(order)
    seqs = flat.shape[0] // cols
    q, _, _ = places(ratio)
    flat[...] = tree([wide(r) for r in right_in])
    for n, k in enumerate(order):
        place = pl.ds(pl.multiple_of((q ^ k ^ (cols - 1)) * seqs, seqs), seqs)
        row = n * seqs % outs[0].shape[0]
        outs[n * 2 // cols][row : row + seqs] = flat[place, :].astype(BF16)


def first_stat_kernel(ratio, *refs):
    proj_in, stat_in = refs[:ratio], refs[ratio : 2 * ratio]
    outs, scratch = refs[2 * ratio : -1], refs[-1]
    height = scratch.shape[1]
    q, _, _ = places(ratio)
    scratch[...] = tree([wide(r) for r in proj_in])
    stat = tree([wide(r) for r in stat_in]).astype(BF16)
    for k, out in enumerate(outs):
        out[:height] = scratch[q ^ k].astype(BF16)
        out[height:] = stat


def second_stat_kernel(ratio, height, *refs):
    count = (len(refs) - 1) // 2
    ins, outs, scratch = refs[:count], refs[count : 2 * count], refs[-1]
    _, _, z = places(ratio)
    total = tree([wide(r) for r in ins])
    size = height * count
    scratch[...] = total[:size].reshape(scratch.shape)
    stat = total[size:].astype(BF16)
    for k, out in enumerate(outs):
        out[:height] = scratch[z ^ k].astype(BF16)
        out[height:] = stat


def last_stat_kernel(chans, height, scale, *refs):
    ins, (gain_ref, lw_ref, rw_ref) = refs[:-8], refs[-8:-5]
    left_ref, right_ref, proj_ref, norm_ref, bias_ref = refs[-5:]
    total = tree([wide(r) for r in ins]) * scale
    proj_ref[...] = total[:height]
    stat = total[height:]
    width = lw_ref.shape[1]
    size = 2 * chans
    halves = width // LANES
    moment = jnp.concatenate([stat[k * size : (k + 1) * size] for k in range(halves)], axis=1)
    left, right = moment[:chans], moment[chans:]
    norm_ref[...] = jnp.sum(left * wide(lw_ref) + right * wide(rw_ref), axis=0, keepdims=True)
    left_ref[...] = left * gain_ref[...]
    right_ref[...] = right * gain_ref[...]
    bias_ref[...] = stat[halves * size : halves * size + 1]


def whole_step(x, gain, left_w, right_w, out_w, bias, cot):
    seqs, residues, width = x.shape
    chans = left_w.shape[1]
    pair_w = out_w.shape[1]
    rows, cols = lax.axis_size("row"), lax.axis_size("col")
    ratio = rows // cols
    seconds = residues * ratio
    total_seqs, total_res = seqs * cols, residues * rows
    wide_proj, wide_pair = residues * chans, seconds * chans
    pack = LANES // chans
    groups = seconds // pack
    gain_row = gain.reshape(1, width)
    left_t, right_t = left_w.T, right_w.T

    def cols_of(parts):
        pairs = [[(i, i ^ k) for i in range(cols)] for k in range(cols)]
        return [parts[0]] + [lax.ppermute(parts[k], "col", pairs[k]) for k in range(1, cols)]

    def chips_of(parts):
        pairs = [[(i, i ^ (k * ratio)) for i in range(rows)] for k in range(cols)]
        return [parts[0]] + [lax.ppermute(parts[k], "row", pairs[k]) for k in range(1, cols)]

    def cores_of(parts):
        pairs = [[(i, i ^ e) for i in range(rows)] for e in range(ratio)]
        return [parts[0]] + [lax.ppermute(parts[e], "row", pairs[e]) for e in range(1, ratio)]

    up = [1 << n for n in range(cols.bit_length() - 1)]
    down = up[::-1]
    pairs = [
        ((q * ratio + h) * cols + z, ((z ^ (cols - 1)) * ratio + h) * cols + q)
        for q in range(cols)
        for h in range(ratio)
        for z in range(cols)
    ]

    sources = (x, gain_row, left_t, right_t, cot, out_w, bias.reshape(1, pair_w))
    outs = call(
        functools.partial(project_kernel, chans),
        sources,
        [(a.shape, a.dtype) for a in sources]
        + [((seqs, wide_proj), BF16)] * 2
        + [((residues * seqs, width), BF16), ((wide_proj, wide_proj), BF16)],
        [
            pltpu.VMEM((width // LANES, seqs * residues, LANES), F32),
            pltpu.SemaphoreType.DMA((len(sources),)),
        ],
        flops=40_000_000,
        far=len(sources),
    )
    x, gain_row, left_t, right_t, cot, out_w, bias_row = outs[: len(sources)]
    left_own, right_own, normed, order = outs[len(sources) :]
    right_own = lax.ppermute(right_own, ("row", "col"), pairs)
    left_in = cols_of([left_own] * cols)
    og, cotk, bias_part = call(
        functools.partial(grad_kernel, chans),
        (cot, out_w),
        [
            ((chans * residues, wide_pair), BF16),
            ((pack * groups * residues, pair_w), BF16),
            ((8, pair_w), F32),
        ],
        [pltpu.VMEM((residues * seconds, pair_w), F32)],
        flops=540_000_000,
    )
    right_in = []
    for chip in chips_of([right_own] * cols):
        right_in += cores_of([chip] * ratio)

    outs = call(
        functools.partial(right_grad_kernel, cols, ratio),
        (*left_in, og),
        [((total_seqs, wide_proj), BF16)] * (ratio + 1),
        [
            pltpu.VMEM((total_seqs, wide_proj), F32),
            pltpu.VMEM((ratio, total_seqs, wide_proj), F32),
        ],
        flops=134_000_000,
    )
    right_parts, left_all = outs[:ratio], outs[ratio]
    kept, moved = call(
        functools.partial(core_sum_kernel, order_of(up), ratio),
        cores_of(right_parts),
        [((total_seqs // 2, wide_proj), BF16)] * 2,
        [pltpu.VMEM((total_seqs, wide_proj), F32)],
    )
    for bit in down:
        moved = lax.ppermute(moved, "row", [(i, i ^ (bit * ratio)) for i in range(rows)])
        shape = ((seqs * max(bit // 2, 1), wide_proj), BF16)
        outs_of = [shape] * (2 if bit > 1 else 1)
        parts = call(split_kernel, (kept, moved), outs_of)
        kept, moved = parts[0], parts[-1]
    right_sent = kept
    right_d = lax.ppermute(right_sent, ("row", "col"), [(b, a) for a, b in pairs])

    outs = call(
        functools.partial(left_grad_kernel, cols, ratio),
        (*right_in, og),
        [((seqs, wide_proj), BF16)] * cols + [((ratio, total_seqs, wide_proj), BF16)],
        [
            pltpu.VMEM((ratio, total_seqs, wide_proj), F32),
            pltpu.VMEM((total_seqs, wide_proj), F32),
        ],
        flops=134_000_000,
    )
    left_parts, right_all = outs[:cols], outs[cols]
    left_parts = cols_of(left_parts)

    block = chans * chans // rows
    outs = call(
        functools.partial(forward_kernel, chans, ratio),
        (left_all, right_all, cotk, out_w, bias_row),
        [((residues, seconds, pair_w), BF16)] + [((cols, block, pair_w), BF16)] * ratio,
        [
            pltpu.VMEM((residues * seconds, pair_w), F32),
            pltpu.VMEM((chans * LANES, pack * pair_w), BF16),
            pltpu.VMEM((groups * residues, chans * LANES), BF16),
            pltpu.VMEM((chans * chans, pack * groups * residues), BF16),
            pltpu.VMEM((cols, ratio, block, pair_w), F32),
        ],
        flops=800_000_000,
        limit=32,
    )
    pair_update, proj_parts = outs[0], outs[1:]
    proj_core = cores_of(proj_parts)

    stat_rows = 2 * chans * (width // LANES) + 8
    left_d, stat = call(
        functools.partial(moment_kernel, cols, chans),
        (*left_parts, right_d, normed, order, bias_part),
        [((seqs, wide_proj), BF16), ((stat_rows, LANES), BF16)],
    )
    stat_core = cores_of([stat] * ratio)
    firsts = call(
        functools.partial(first_stat_kernel, ratio),
        (*proj_core, *stat_core),
        [((block + stat_rows, pair_w), BF16)] * cols,
        [pltpu.VMEM((cols, block, pair_w), F32)],
    )
    firsts = chips_of(firsts)
    height = block // cols
    seconds_out = call(
        functools.partial(second_stat_kernel, ratio, height),
        firsts,
        [((height + stat_rows, pair_w), BF16)] * cols,
        [pltpu.VMEM((cols, height, pair_w), F32)],
    )
    seconds_out = cols_of(seconds_out)
    grad = call(
        functools.partial(input_grad_kernel, chans),
        (x, gain_row, left_t, right_t, left_d, right_d),
        [((seqs, residues, width), BF16)],
        [pltpu.VMEM((width // LANES, seqs * residues, LANES), F32)],
    )[0]
    left_g, right_g, proj_g, norm_g, bias_g = call(
        functools.partial(last_stat_kernel, chans, height, 1.0 / total_res),
        (*seconds_out, gain_row, left_t, right_t),
        [
            ((chans, width), F32),
            ((chans, width), F32),
            ((height, pair_w), F32),
            ((1, width), F32),
            ((1, pair_w), F32),
        ],
    )
    return (
        pair_update,
        grad,
        left_g.T,
        right_g.T,
        proj_g,
        norm_g.reshape(width),
        bias_g.reshape(pair_w),
    )


def solution(mesh):
    return jax.shard_map(
        whole_step,
        mesh=mesh,
        in_specs=(P("col", "row", None), P(), P(), P(), P(), P(), P("row", "col", None)),
        out_specs=(
            P("row", "col", None),
            P("col", "row", None),
            P(),
            P(),
            P(("row", "col"), None),
            P(),
            P(),
        ),
        check_vma=False,
    )
```
